1024 devices in a mesh: row: 16 (over x, z_hi), col: 64 (over y, z_lo, core).
Axes of the slice: x: 8, y: 8, z: 8 (z_hi: 2, z_lo: 4; z = z_hi * 4 + z_lo), core: 2. Of those that a mesh axis runs over, the one named last changes fastest.
Arguments:
- pair_states: bfloat16 [1024, 16384], P(None, ('row', 'col')), may hold values from -0.046875 to 0.046875
- screening: bfloat16 [4, 16384, 16384], P(None, 'row', 'col'), may hold values from -6 to 6
- qp_energy: float32 [8], replicated, may hold values from -0.5 to 0.5
- band_energy: float32 [2048], replicated, may hold values from -2 to 2
- band_index: int32 [128], replicated, may hold values from 0 to 2047
- nodes: float32 [4], replicated, may hold values from 0.1 to 2
- node_weights: float32 [4], replicated, may hold values from 0.05 to 1
Outputs:
- contrib: float32 [8, 128], replicated
- sigma: float32 [8], replicated
The draws below stay inside these ranges and needn't reach their ends.
All inputs are finite; a program needn't handle non-finite values.
Results may differ from the reference program's by a relative error of at most 0.0003.
Values may be sent and summed in bfloat16 or wider, within the bound.
No kernel may reach another device: no remote copies, remote signals or barrier semaphores. Data moves between devices by JAX's collectives and lax.ppermute only.
A program may use at most 64 MiB of HBM per device.

```python
import math
import jax
import jax.numpy as jnp
from jax import lax

NG = 16384
FREQS = 4
NQ = 8
NM = 128
NBANDS = 2048
PAIRS = 1024


def plant(result, rng, least, top_value):
    dims = result.shape
    place = [jax.random.randint(jax.random.fold_in(rng, axis), (), 0, dims[axis]) for axis in range(len(dims))]
    result = result.at[tuple(place)].set(least)
    longest = dims.index(max(dims))
    place[longest] = (place[longest] + 1) % dims[longest]
    return result.at[tuple(place)].set(top_value)


def levels(rng, extent, cuts, least, largest):
    gain, own = 1.0, jax.random.fold_in(rng, 6)
    for axis_at, shards_of in cuts:
        heights = jnp.exp(jax.random.uniform(jax.random.fold_in(own, axis_at), (shards_of,), jnp.float32, least / len(cuts), largest / len(cuts)))
        gain = gain * jnp.repeat(heights, extent[axis_at] // shards_of).reshape([-1 if axis == axis_at else 1 for axis in range(len(extent))])
    return gain


def noise(rng, dims, width, reach, pieces=(), held_as=jnp.bfloat16):
    values = jax.random.normal(rng, dims, jnp.float32) * width
    if len(pieces) > 0:
        values = levels(rng, dims, pieces, -0.22, 0.18) * values
    return jnp.clip(values, min=-reach, max=reach).astype(held_as)


def setup_inputs(seed: int = 0) -> dict:
    key_of = jax.random.split(jax.random.key(seed), 8)
    return {
        "pair_states": noise(key_of[0], (PAIRS, NG), NG ** -0.5, 0.046875, ((1, 1024),)),
        "screening": noise(key_of[1], (FREQS, NG, NG), 1.0, 6.0, ((1, 16), (2, 64))),
        "qp_energy": jnp.clip(jax.random.uniform(key_of[2], (NQ,), jnp.float32, -0.5, 0.5), -0.5, 0.5),
        "band_energy": jnp.clip(jax.random.uniform(key_of[3], (NBANDS,), jnp.float32, -2.0, 2.0), -2.0, 2.0),
        "band_index": plant(jax.random.randint(key_of[4], (NM,), 0, NBANDS), jax.random.fold_in(key_of[4], 1), 0, NBANDS - 1).astype(jnp.int32),
        "nodes": jnp.clip(jnp.exp(jax.random.uniform(key_of[5], (FREQS,), jnp.float32, math.log(0.1), math.log(2.0))), 0.1, 2.0),
        "node_weights": jnp.clip(jnp.exp(jax.random.uniform(key_of[6], (FREQS,), jnp.float32, math.log(0.05), math.log(1.0))), 0.05, 1.0),
    }


def reference(pair_states, screening, qp_energy, band_energy, band_index, nodes, node_weights):
    states = pair_states.astype(jnp.float32)

    def one_node(layer):
        image = jnp.dot(states, layer.astype(jnp.float32), precision=lax.Precision.HIGHEST, preferred_element_type=jnp.float32)
        return jnp.sum(image * states, axis=1)

    quad = lax.map(one_node, screening)
    table = jnp.arange(NBANDS).astype(jnp.int32)
    chosen = jnp.sum(jnp.where(band_index[:, None] == table[None, :], band_energy[None, :], jnp.float32(0.0)), axis=1)
    gap = (qp_energy[:, None] - chosen[None, :]).reshape(-1)
    factor = node_weights[:, None] * gap[None, :] / (gap[None, :] * gap[None, :] + nodes[:, None] * nodes[:, None])
    contrib = jnp.sum(factor * quad, axis=0).reshape(NQ, NM)
    sigma = jnp.sum(contrib, axis=1)
    return contrib, sigma
```

```python
import jax
import jax.numpy as jnp
from jax import lax
from jax.experimental import pallas as pl
from jax.experimental.pallas import tpu as pltpu
from jax.sharding import Mesh
from jax.sharding import PartitionSpec as P

AXES = ("x", "zh", "yh", "yl", "zlh", "zll", "core")
SIZES = (8, 2, 4, 2, 2, 2, 2)
ROW = ("x", "zh")
COL = ("yh", "yl", "zlh", "zll", "core")
FAR = ("yh", "zlh")
NEAR = ("yl", "zll")


def sent_to_all(array, axes):
    copies = jnp.broadcast_to(array, (lax.axis_size(axes), *array.shape))
    return lax.all_to_all(copies, axes, split_axis=0, concat_axis=0, tiled=True)


def transposed_place():
    return [(b, (b % 16) * 64 + b // 16) for b in range(1024)]


def contract(w_ref, col_ref, row_ref, factor_ref, base_ref, out_ref):
    total = jnp.zeros((8, 1024), jnp.float32)
    for yh in range(4):
        for yl in range(2):
            k = (yh * 2 + yl) * 64
            weighted = jnp.zeros((64, 1024), jnp.float32)
            for f in range(4):
                image = jnp.dot(w_ref[f, k : k + 64, :], col_ref[...], preferred_element_type=jnp.float32)
                weighted += image * factor_ref[f : f + 1, :]
            for zlh in range(2):
                for zll in range(2):
                    part = weighted[(zlh * 2 + zll) * 16 : (zlh * 2 + zll) * 16 + 16, :]
                    states = row_ref[yl * 2 + zll, yh * 2 + zlh, :, :].astype(jnp.float32)
                    product = part * states
                    total += product[:8] + product[8:]
    for n in range(8):
        out_ref[n : n + 1, :] = base_ref[n : n + 1, :] + jnp.sum(total[:, n * 128 : n * 128 + 128], axis=0, keepdims=True)


def contracted(w, col, row, factor, base):
    return pl.pallas_call(
        contract,
        out_shape=jax.ShapeDtypeStruct((8, 128), jnp.float32),
        in_specs=[pl.BlockSpec(memory_space=pltpu.VMEM)] * 5,
        out_specs=pl.BlockSpec(memory_space=pltpu.VMEM),
        cost_estimate=pl.CostEstimate(flops=2 * 4 * 512 * 256 * 1024, bytes_accessed=2 << 20, transcendentals=0),
    )(w, col, row, factor, base)


def shards(pair_states, screening, qp_energy, band_energy, band_index, nodes, node_weights):
    piece = pair_states.T
    moved = lax.ppermute(piece, ROW + COL, transposed_place())
    table = lax.broadcasted_iota(jnp.int32, (band_index.shape[0], band_energy.shape[0]), 1)
    chosen = jnp.sum(
        jnp.where(band_index[:, None] == table, band_energy[None, :], jnp.float32(0.0)), axis=1
    )
    gap = (qp_energy[:, None] - chosen[None, :]).reshape(-1)
    factor = (
        node_weights[:, None]
        * gap[None, :]
        / (gap[None, :] * gap[None, :] + nodes[:, None] * nodes[:, None])
    )
    far = sent_to_all(piece, FAR)
    near = sent_to_all(far, NEAR)
    other = lax.ppermute(near, "core", [(0, 1), (1, 0)])
    col = sent_to_all(moved, ROW).reshape(256, 1024)
    core = lax.axis_index("core")
    w = screening.reshape(4, 32, 2, 16, 256)
    own_w = lax.dynamic_index_in_dim(w, core, 2, keepdims=False).reshape(4, 512, 256)
    other_w = lax.dynamic_index_in_dim(w, 1 - core, 2, keepdims=False).reshape(4, 512, 256)
    partial_value = contracted(own_w, col, near, factor, jnp.zeros((8, 128), jnp.float32))
    partial_value = contracted(other_w, col, other, factor, partial_value)
    for axes in (("x", "core"), ("yh", "yl"), ("zh", "zlh", "zll")):
        partial_value = jnp.sum(sent_to_all(partial_value, axes), axis=0)
    sigma = jnp.sum(partial_value, axis=1)
    return (partial_value, sigma)


def solution(mesh):
    split = Mesh(mesh.devices.reshape(SIZES), AXES)
    return jax.shard_map(
        shards,
        mesh=split,
        in_specs=(P(None, ROW + COL), P(None, ROW, COL), P(), P(), P(), P(), P()),
        out_specs=(P(), P()),
        check_vma=False,
    )
```

```python
import jax
import jax.numpy as jnp
from jax import lax
from jax.experimental import pallas as pl
from jax.experimental.pallas import tpu as pltpu
from jax.sharding import Mesh
from jax.sharding import PartitionSpec as P

AXES = ("x", "zh", "y", "zl", "core")
SIZES = (8, 2, 8, 4, 2)
ROW = ("x", "zh")
COL = ("y", "zl", "core")
VMEM = pl.BlockSpec(memory_space=pltpu.VMEM)


def sent_to_all(array, axes):
    copies = jnp.broadcast_to(array, (lax.axis_size(axes), *array.shape))
    return lax.all_to_all(copies, axes, split_axis=0, concat_axis=0, tiled=True)


def transposed_place():
    return [(b, (b % 16) * 64 + b // 16) for b in range(1024)]


def weigh(has_base, w_ref, row_ref, factor_ref, *refs):
    out_ref = refs[-1]
    for k in range(0, 1024, 256):
        states = row_ref[:, k : k + 256]
        total = refs[0][:, k : k + 256] if has_base else None
        for f in range(4):
            image = jnp.dot(w_ref[f], states, preferred_element_type=jnp.float32)
            term = image * factor_ref[f : f + 1, k : k + 256]
            total = term if total is None else total + term
        out_ref[:, k : k + 256] = total


def weighed(w, row, factor, *base):
    return pl.pallas_call(
        lambda *refs: weigh(len(base) > 0, *refs),
        out_shape=jax.ShapeDtypeStruct((256, 1024), jnp.float32),
        in_specs=[VMEM] * (3 + len(base)),
        out_specs=VMEM,
        cost_estimate=pl.CostEstimate(flops=2 * 4 * 512 * 256 * 1024, bytes_accessed=4 << 20, transcendentals=0),
    )(w, row, factor, *base)


def project(weighed_ref, col_ref, out_ref):
    for n in range(8):
        part = slice(n * 128, n * 128 + 128)
        total = jnp.sum(weighed_ref[:, part] * col_ref[:, part].astype(jnp.float32), axis=0, keepdims=True)
        for copy in range(out_ref.shape[0]):
            out_ref[copy, n : n + 1, :] = total


def add(pieces_ref, out_ref):
    total = pieces_ref[0]
    for piece in range(1, pieces_ref.shape[0]):
        total = total + pieces_ref[piece]
    for copy in range(out_ref.shape[0]):
        out_ref[copy] = total


def in_kernel(body, copies, *args):
    return pl.pallas_call(
        body,
        out_shape=jax.ShapeDtypeStruct((copies, 8, 128), jnp.float32),
        in_specs=[VMEM] * len(args),
        out_specs=VMEM,
    )(*args)


def exchanged(copies, axes):
    return lax.all_to_all(copies, axes, split_axis=0, concat_axis=0, tiled=True)


def factors(qp_energy, band_energy, band_index, nodes, node_weights):
    table = lax.broadcasted_iota(jnp.int32, (band_index.shape[0], band_energy.shape[0]), 1)
    chosen = jnp.sum(
        jnp.where(band_index[:, None] == table, band_energy[None, :], jnp.float32(0.0)), axis=1
    )
    gap = (qp_energy[:, None] - chosen[None, :]).reshape(-1)
    return (
        node_weights[:, None]
        * gap[None, :]
        / (gap[None, :] * gap[None, :] + nodes[:, None] * nodes[:, None])
    )


def shards(pair_states, screening, qp_energy, band_energy, band_index, nodes, node_weights):
    piece = pair_states.T
    moved = lax.ppermute(piece, ROW + COL, transposed_place())
    factor = factors(qp_energy, band_energy, band_index, nodes, node_weights)
    core = lax.axis_index("core")
    slabs = screening.reshape(4, 32, 2, 16, 256)
    own_w, other_w = (
        lax.dynamic_index_in_dim(slabs, which, 2, keepdims=False).reshape(4, 512, 256).transpose(0, 2, 1)
        for which in (core, 1 - core)
    )
    row = sent_to_all(piece, ("y", "zl")).reshape(512, 1024)
    other = lax.ppermute(row, "core", [(0, 1), (1, 0)])
    col = sent_to_all(moved, ROW).reshape(256, 1024)
    weighted = weighed(own_w, row, factor)
    weighted = weighed(other_w, other, factor, weighted)
    copies = in_kernel(project, 16, weighted, col)
    copies = in_kernel(add, 64, exchanged(copies, ("zh", "zl", "core")))
    contrib = in_kernel(add, 1, exchanged(copies, ("x", "y")))[0]
    sigma = jnp.sum(contrib, axis=1)
    return (contrib, sigma)


def solution(mesh):
    split = Mesh(mesh.devices.reshape(SIZES), AXES)
    return jax.shard_map(
        shards,
        mesh=split,
        in_specs=(P(None, ROW + COL), P(None, ROW, COL), P(), P(), P(), P(), P()),
        out_specs=(P(), P()),
        check_vma=False,
    )
```

```python
import jax
import jax.numpy as jnp
from jax import lax
from jax.experimental import pallas as pl
from jax.experimental.pallas import tpu as pltpu
from jax.sharding import Mesh
from jax.sharding import PartitionSpec as P

AXES = ("x", "zh", "yh", "yl", "zlh", "zll", "core")
SIZES = (8, 2, 4, 2, 2, 2, 2)
ROW = ("x", "zh")
COL = ("yh", "yl", "zlh", "zll", "core")
NEAR = ("yl", "zll")


def sent_to_all(array, axes):
    copies = jnp.broadcast_to(array, (lax.axis_size(axes), *array.shape))
    return lax.all_to_all(copies, axes, split_axis=0, concat_axis=0, tiled=True)


def transposed_place(flip):
    return [(b, (b % 16 ^ flip) * 64 + b // 16) for b in range(1024)]


def weigh(block_ref, w_ref, own_ref, other_ref, factor_ref, out_ref, held_ref):
    @pl.when(pl.program_id(0) == 0)
    def _():
        for j in range(8):
            for f in range(4):
                held_ref[f, :, j * 128 : j * 128 + 128] = w_ref[block_ref[j], f]

    total = None
    for f in range(4):
        image = jnp.dot(held_ref[f, :, :512], own_ref[...], preferred_element_type=jnp.float32)
        image += jnp.dot(held_ref[f, :, 512:], other_ref[...], preferred_element_type=jnp.float32)
        term = image * factor_ref[f : f + 1, :]
        total = term if total is None else total + term
    out_ref[...] = total


def weighed(block, w, own, other, factor):
    return pl.pallas_call(
        weigh,
        grid=(4,),
        out_shape=jax.ShapeDtypeStruct((256, 1024), jnp.float32),
        in_specs=[
            pl.BlockSpec(memory_space=pltpu.SMEM),
            pl.BlockSpec((8, 4, 256, 128), lambda i: (0, 0, 0, 0)),
            pl.BlockSpec((512, 256), lambda i: (0, i)),
            pl.BlockSpec((512, 256), lambda i: (0, i)),
            pl.BlockSpec((4, 256), lambda i: (0, i)),
        ],
        out_specs=pl.BlockSpec((256, 256), lambda i: (0, i)),
        scratch_shapes=[pltpu.VMEM((4, 256, 1024), jnp.bfloat16)],
        cost_estimate=pl.CostEstimate(flops=2 * 4 * 1024 * 256 * 1024, bytes_accessed=5 << 20, transcendentals=0),
    )(block, w, own, other, factor)


def factors(qp_energy, band_energy, band_index, nodes, node_weights):
    table = lax.broadcasted_iota(jnp.int32, (band_index.shape[0], band_energy.shape[0]), 1)
    chosen = jnp.sum(
        jnp.where(band_index[:, None] == table, band_energy[None, :], jnp.float32(0.0)), axis=1
    )
    gap = (qp_energy[:, None] - chosen[None, :]).reshape(-1)
    return (
        node_weights[:, None]
        * gap[None, :]
        / (gap[None, :] * gap[None, :] + nodes[:, None] * nodes[:, None])
    )


def shards(pair_states, screening, qp_energy, band_energy, band_index, nodes, node_weights):
    piece = pair_states.T
    far = sent_to_all(piece, ("yh", "zlh")).reshape(128, 1024)
    moved = [lax.ppermute(piece, ROW + COL, transposed_place(zh)) for zh in range(2)]
    near = [far] + [lax.ppermute(far, NEAR, [(n, n ^ d) for n in range(4)]) for d in range(1, 4)]
    own = jnp.concatenate(near)
    other = lax.ppermute(own, "core", [(0, 1), (1, 0)])
    factor = factors(qp_energy, band_energy, band_index, nodes, node_weights)
    w = screening.reshape(4, 4, 2, 2, 2, 2, 16, 256).transpose(2, 4, 5, 0, 7, 1, 3, 6).reshape(8, 4, 256, 128)
    core, place = lax.axis_index("core"), lax.axis_index(NEAR)
    which = lax.iota(jnp.int32, 8)
    block = (place ^ (which % 4)) * 2 + (core ^ (which // 4))
    moved = jnp.where(lax.axis_index("zh") == 0, jnp.stack(moved), jnp.stack(moved[::-1]))
    col = sent_to_all(moved, "x").reshape(256, 1024)
    weighted = weighed(block, w, own, other, factor)
    contrib = jnp.sum(weighted * col.astype(jnp.float32), axis=0).reshape(8, 128)
    for axes in (("x", "core"), ("yh", "yl"), ("zh", "zlh", "zll")):
        contrib = jnp.sum(sent_to_all(contrib, axes), axis=0)
    sigma = jnp.sum(contrib, axis=1)
    return (contrib, sigma)


def solution(mesh):
    split = Mesh(mesh.devices.reshape(SIZES), AXES)
    return jax.shard_map(
        shards,
        mesh=split,
        in_specs=(P(None, ROW + COL), P(None, ROW, COL), P(), P(), P(), P(), P()),
        out_specs=(P(), P()),
        check_vma=False,
    )
```

```python
import jax
import jax.numpy as jnp
from jax import lax
from jax.experimental import pallas as pl
from jax.experimental.pallas import tpu as pltpu
from jax.sharding import Mesh
from jax.sharding import PartitionSpec as P

AXES = ("x", "zh", "yh", "yl", "zlh", "zll", "core")
SIZES = (8, 2, 4, 2, 2, 2, 2)
ROW = ("x", "zh")
COL = ("yh", "yl", "zlh", "zll", "core")
NEAR = ("yl", "zll")


def sent_to_all(array, axes):
    copies = jnp.broadcast_to(array, (lax.axis_size(axes), *array.shape))
    return lax.all_to_all(copies, axes, split_axis=0, concat_axis=0, tiled=True)


def transposed_place(flip):
    return [(b, (b % 16 ^ flip) * 64 + b // 16) for b in range(1024)]


def weigh(has_base, nodes_ref, weights_ref, w_ref, row_ref, gap_ref, *refs):
    out_ref, held_ref, sum_ref, states_ref, sems = refs[-5:]
    place = lax.axis_index(NEAR)
    copies = [pltpu.make_async_copy(row_ref.at[place ^ n], states_ref.at[n], sems.at[n]) for n in range(4)]

    @pl.when(pl.program_id(0) == 0)
    def _():
        for copy in copies:
            copy.start()

    for f in range(4):
        for zll in range(2):
            slabs = [w_ref[f, yh, 0, zlh, zll, 0] for yh in range(4) for zlh in range(2)]
            held_ref[f, :, zll * 128 : zll * 128 + 128] = jnp.concatenate(slabs, axis=0).T

    def added(base_ref, yl, k):
        gap = gap_ref[:, k : k + 256]
        states = jnp.concatenate([states_ref[2 * yl, :, k : k + 256], states_ref[2 * yl + 1, :, k : k + 256]], axis=0)
        total = None if base_ref is None else base_ref[:, k : k + 256]
        for f in range(4):
            image = jnp.dot(held_ref[f], states, preferred_element_type=jnp.float32)
            term = image * (weights_ref[f] * gap / (gap * gap + nodes_ref[f] * nodes_ref[f]))
            total = term if total is None else total + term
        return total

    @pl.when(pl.program_id(0) == 0)
    def _():
        for copy in copies[:2]:
            copy.wait()
        for k in range(0, 1024, 256):
            sum_ref[:, k : k + 256] = added(refs[0] if has_base else None, 0, k)

    @pl.when(pl.program_id(0) == 1)
    def _():
        for copy in copies[2:]:
            copy.wait()
        for k in range(0, 1024, 256):
            out_ref[:, k : k + 256] = added(sum_ref, 1, k)


def weighed(flip, w, row, gap, nodes, node_weights, *base):
    row = row.reshape(4, 128, 1024)
    whole = pl.BlockSpec((256, 1024), lambda i, *_: (0, 0))
    return pl.pallas_call(
        lambda *refs: weigh(len(base) > 0, *refs),
        grid_spec=pltpu.PrefetchScalarGridSpec(
            num_scalar_prefetch=2,
            grid=(2,),
            in_specs=[
                pl.BlockSpec((4, 4, 1, 2, 2, 1, 16, 256), lambda i, *_: (0, 0, i, 0, 0, lax.axis_index("core") ^ flip, 0, 0)),
                pl.BlockSpec(memory_space=pl.ANY),
                pl.BlockSpec((1, 1024), lambda i, *_: (0, 0)),
            ]
            + [whole] * len(base),
            out_specs=whole,
            scratch_shapes=[
                pltpu.VMEM((4, 256, 256), jnp.bfloat16),
                pltpu.VMEM((256, 1024), jnp.float32),
                pltpu.VMEM((4, 128, 1024), jnp.bfloat16),
                pltpu.SemaphoreType.DMA((4,)),
            ],
        ),
        out_shape=jax.ShapeDtypeStruct((256, 1024), jnp.float32),
        compiler_params=pltpu.CompilerParams(vmem_limit_bytes=16 << 20),
        cost_estimate=pl.CostEstimate(flops=2 * 4 * 512 * 256 * 1024, bytes_accessed=4 << 20, transcendentals=0),
    )(nodes, node_weights, w, row, gap, *base)


def gaps(qp_energy, band_energy, band_index):
    table = lax.broadcasted_iota(jnp.int32, (band_index.shape[0], band_energy.shape[0]), 1)
    chosen = jnp.sum(
        jnp.where(band_index[:, None] == table, band_energy[None, :], jnp.float32(0.0)), axis=1
    )
    gap = (qp_energy[:, None] - chosen[None, :]).reshape(-1)
    return gap[None, :]


def shards(pair_states, screening, qp_energy, band_energy, band_index, nodes, node_weights):
    piece = pair_states.T
    moved = [lax.ppermute(piece, ROW + COL, transposed_place(0))]
    far = sent_to_all(piece, ("yh", "zlh")).reshape(128, 1024)
    moved.append(lax.ppermute(piece, ROW + COL, transposed_place(1)))
    near = [far] + [lax.ppermute(far, NEAR, [(n, n ^ d) for n in range(4)]) for d in range(1, 4)]
    own = jnp.concatenate(near)
    other = lax.ppermute(own, "core", [(0, 1), (1, 0)])
    gap = gaps(qp_energy, band_energy, band_index)
    w = screening.reshape(4, 4, 2, 2, 2, 2, 16, 256)
    moved = jnp.where(lax.axis_index("zh") == 0, jnp.stack(moved), jnp.stack(moved[::-1]))
    col = sent_to_all(moved, "x").reshape(256, 1024)
    weighted = weighed(0, w, own, gap, nodes, node_weights)
    weighted = weighed(1, w, other, gap, nodes, node_weights, weighted)
    contrib = jnp.sum(weighted * col.astype(jnp.float32), axis=0).reshape(8, 128)
    for axes in (("x", "core"), ("yh", "yl"), ("zh", "zlh", "zll")):
        contrib = jnp.sum(sent_to_all(contrib, axes), axis=0)
    sigma = jnp.sum(contrib, axis=1)
    return (contrib, sigma)


def solution(mesh):
    split = Mesh(mesh.devices.reshape(SIZES), AXES)
    return jax.shard_map(
        shards,
        mesh=split,
        in_specs=(P(None, ROW + COL), P(None, ROW, COL), P(), P(), P(), P(), P()),
        out_specs=(P(), P()),
        check_vma=False,
    )
```
